32 devices in a mesh: dp: 16 (over z, x, core), tensor: 2 (over y).
Axes of the slice: x: 2, y: 2, z: 4, core: 2. Of those that a mesh axis runs over, the one named last changes fastest.
Arguments:
- states: float32 [24576, 1536], P(('dp', 'tensor')), may hold values from -6 to 6
- text_states: float32 [16, 64, 1536], P('dp'), may hold values from -6 to 6
- norm_gains: float32 [3, 1536], P(None, 'dp'), may hold values from 0.25 to 1.75
- norm_biases: float32 [3, 1536], P(None, 'dp'), may hold values from -3 to 3
- self_qkv: float32 [1536, 3, 1536], P('dp', None, 'tensor'), may hold values from -0.15625 to 0.15625
- self_out: float32 [1536, 1536], P('tensor', 'dp'), may hold values from -1.25 to 1.25
- cross_query: float32 [1536, 1536], P('dp', 'tensor'), may hold values from -0.15625 to 0.15625
- cross_kv: float32 [1536, 2, 1536], P('dp', None, 'tensor'), may hold values from -0.15625 to 0.15625
- cross_out: float32 [1536, 1536], P('tensor', 'dp'), may hold values from -1.25 to 1.25
- mlp_up: float32 [1536, 6144], P('dp', 'tensor'), may hold values from -0.15625 to 0.15625
- mlp_down: float32 [6144, 1536], P('tensor', 'dp'), may hold values from -0.078125 to 0.078125
- out_grad: float32 [24576, 1536], P(('dp', 'tensor')), may hold values from -6 to 6
Outputs:
- layer_out: float32 [24576, 1536], P(('dp', 'tensor'))
- states_grad: float32 [24576, 1536], P(('dp', 'tensor'))
- text_grad: float32 [16, 64, 1536], P('dp')
- gains_grad: float32 [3, 1536], P(None, 'dp')
- biases_grad: float32 [3, 1536], P(None, 'dp')
- self_qkv_grad: float32 [1536, 3, 1536], P('dp', None, 'tensor')
- self_out_grad: float32 [1536, 1536], P('tensor', 'dp')
- cross_query_grad: float32 [1536, 1536], P('dp', 'tensor')
- cross_kv_grad: float32 [1536, 2, 1536], P('dp', None, 'tensor')
- cross_out_grad: float32 [1536, 1536], P('tensor', 'dp')
- mlp_up_grad: float32 [1536, 6144], P('dp', 'tensor')
- mlp_down_grad: float32 [6144, 1536], P('tensor', 'dp')
The draws below stay inside these ranges and needn't reach their ends.
All inputs are finite; a program needn't handle non-finite values.
Results may differ from the reference program's by a relative error of at most 0.017.
The reference program's roundings to bfloat16 on the way count: a program that leaves them out, or rounds other values in their place, can miss the bound.
Values may be sent and summed in bfloat16 or wider, within the bound.
A program may use at most 384 MiB of HBM per device.

```python
import math
import jax
import jax.numpy as jnp
from jax import lax

D = 1536
HEADS = 24
HEAD_DIM = 64
FF = 6144
TEXT = 64
FRAMES = 1536
CLIPS = 16
TOKENS = 24576


def strengthened(values, stream_key, source, target, shards_of, factor):
    owner, partner = [(jnp.arange(values.shape[dim]) // (values.shape[dim] // shards_of)).reshape([-1 if axis == dim else 1 for axis in range(values.ndim)]) for dim in (source, target)]
    chosen = jax.random.permutation(stream_key, shards_of)[partner]
    strong = (owner == chosen) | (owner == (partner + shards_of // 2) % shards_of)
    return jnp.where(strong, factor * values, values)


def shard_levels(stream_key, dims, pieces, smallest, largest):
    def one(axis_at, blocks):
        draws = jax.random.uniform(jax.random.fold_in(jax.random.fold_in(stream_key, 6), axis_at), (blocks,), jnp.float32, smallest / len(pieces), largest / len(pieces))
        return jnp.repeat(jnp.exp(draws), dims[axis_at] // blocks).reshape((-1,) + (1,) * (len(dims) - axis_at - 1))

    loudness = one(*pieces[0])
    for cut in pieces[1:]:
        loudness = loudness * one(*cut)
    return loudness


def scatter_about(stream_key, extent, width, limit, pieces=(), held_as=jnp.bfloat16):
    loudness = shard_levels(stream_key, extent, pieces, -0.22, 0.18) if pieces else 1.0
    drawn = jax.random.normal(stream_key, extent, jnp.float32) * width * loudness
    return jnp.minimum(jnp.maximum(drawn, -limit), limit).astype(held_as)


def bell_draw_with(stream_key, shape, scale, most, cuts, heavy, held_as=jnp.bfloat16):
    drawn = scale * jax.random.normal(stream_key, shape, jnp.float32)
    if cuts:
        drawn = drawn * shard_levels(stream_key, shape, cuts, -0.22, 0.18)
    return jnp.clip(strengthened(drawn, jax.random.fold_in(stream_key, 3), *heavy), -most, most).astype(held_as)


def setup_inputs(seed: int = 0) -> dict:
    key_of = jax.random.split(jax.random.key(seed), 13)
    return {
        "states": scatter_about(key_of[0], (TOKENS, D), 1.0, 6.0, ((0, 32),), jnp.float32),
        "text_states": scatter_about(key_of[1], (CLIPS, TEXT, D), 1.0, 6.0, ((0, 16),), jnp.float32),
        "norm_gains": jnp.clip(1.0 + 0.15 * jax.random.normal(key_of[2], (3, D), jnp.float32), 0.25, 1.75),
        "norm_biases": scatter_about(key_of[3], (3, D), 0.5, 3.0, ((1, 16),), jnp.float32),
        "self_qkv": scatter_about(key_of[4], (D, 3, D), D ** -0.5, 0.15625, ((0, 16), (2, 2)), jnp.float32),
        "self_out": scatter_about(key_of[5], (D, D), (max(D // 64, 1)) ** -0.5, 1.25, ((0, 2), (1, 16)), jnp.float32),
        "cross_query": scatter_about(key_of[6], (D, D), D ** -0.5, 0.15625, ((0, 16), (1, 2)), jnp.float32),
        "cross_kv": scatter_about(key_of[7], (D, 2, D), D ** -0.5, 0.15625, ((0, 16), (2, 2)), jnp.float32),
        "cross_out": scatter_about(key_of[8], (D, D), (max(D // 64, 1)) ** -0.5, 1.25, ((0, 2), (1, 16)), jnp.float32),
        "mlp_up": scatter_about(key_of[9], (D, FF), D ** -0.5, 0.15625, ((0, 16), (1, 2)), jnp.float32),
        "mlp_down": scatter_about(key_of[10], (FF, D), FF ** -0.5, 0.078125, ((0, 2), (1, 16)), jnp.float32),
        "out_grad": bell_draw_with(key_of[11], (TOKENS, D), 1.0, 6.0, ((0, 32),), (0, 1, 32, 2.75), jnp.float32),
    }


EPSILON = 1e-05
MASKED = -1e+30
HIGHEST = lax.Precision.HIGHEST

@jax.custom_vjp
def low(v):
    return lax.optimization_barrier(v.astype(jnp.bfloat16)).astype(jnp.float32)

@jax.custom_vjp
def low_back(v):
    return v

def low_keep(v):
    return (low(v), None)

def low_pass(kept, grad):
    return (grad,)

def back_keep(v):
    return (v, None)

def back_low(kept, grad):
    return (low(grad),)
low.defvjp(low_keep, low_pass)
low_back.defvjp(back_keep, back_low)

def rounded_both(values):
    return low_back(low(values))

def layer_norm(values, gain, shift):
    centre = lax.optimization_barrier(jnp.mean(values, axis=-1, keepdims=True))
    centred = values - centre
    spread = lax.optimization_barrier(jnp.mean(centred * centred, axis=-1, keepdims=True))
    return centred * lax.rsqrt(spread + EPSILON) * gain + shift

def split_heads(block):
    return block.reshape(block.shape[0], HEADS, HEAD_DIM)

def attention(queries, keys, values, causal):
    length = queries.shape[0]
    block = min(512, length)
    scale_factor = 1.0 / math.sqrt(HEAD_DIM)

    def one_block(number):
        offset = number * block
        query_block = lax.dynamic_slice_in_dim(queries, offset, block, 0)
        scores = low_back(jnp.einsum('bhe,khe->hbk', query_block, keys, precision=HIGHEST) * scale_factor)
        if causal:
            query_pos = offset + lax.broadcasted_iota(jnp.int32, (block, keys.shape[0]), 0)
            key_pos = lax.broadcasted_iota(jnp.int32, (block, keys.shape[0]), 1)
            scores = jnp.where((key_pos <= query_pos)[None], scores, MASKED)
        probs = jax.nn.softmax(scores, axis=-1)
        return jnp.einsum('hbk,khe->bhe', low(probs), values, precision=HIGHEST)
    mixed = lax.map(jax.checkpoint(one_block), jnp.arange(length // block, dtype=jnp.int32))
    return mixed.reshape(length, HEADS * HEAD_DIM)

def forward(params, values, text):
    gains, biases, w_qkv, w_self_out, w_query, w_kv, w_cross_out, w_up, w_down = [low(item) for item in params]
    normed_one = low(layer_norm(values, gains[0], biases[0]))
    triple = rounded_both(jnp.einsum('td,dkc->tkc', normed_one, w_qkv, precision=HIGHEST))
    self_mixed = rounded_both(attention(split_heads(triple[:, 0]), split_heads(triple[:, 1]), split_heads(triple[:, 2]), True))
    after_self = values + low_back(jnp.dot(self_mixed, w_self_out, precision=HIGHEST))
    normed_two = low(layer_norm(after_self, gains[1], biases[1]))
    cross_queries = rounded_both(jnp.dot(normed_two, w_query, precision=HIGHEST))
    text_low = low(text)
    text_pair = rounded_both(jnp.einsum('td,dkc->tkc', text_low, w_kv, precision=HIGHEST))
    cross_mixed = rounded_both(attention(split_heads(cross_queries), split_heads(text_pair[:, 0]), split_heads(text_pair[:, 1]), False))
    after_cross = after_self + low_back(jnp.dot(cross_mixed, w_cross_out, precision=HIGHEST))
    normed_three = low(layer_norm(after_cross, gains[2], biases[2]))
    hidden_pre = low_back(jnp.dot(normed_three, w_up, precision=HIGHEST))
    hidden = low(jax.nn.gelu(hidden_pre, approximate=False))
    return after_cross + low_back(jnp.dot(hidden, w_down, precision=HIGHEST))

def reference(states, text_states, norm_gains, norm_biases, self_qkv, self_out, cross_query, cross_kv, cross_out, mlp_up, mlp_down, out_grad):
    params = (norm_gains, norm_biases, self_qkv, self_out, cross_query, cross_kv, cross_out, mlp_up, mlp_down)
    clip_rows = states.reshape(CLIPS, FRAMES, D)
    clip_grads = out_grad.reshape(CLIPS, FRAMES, D)

    def clip_step(totals, inputs):
        values, text, cotangent = inputs
        result, pull = jax.vjp(forward, params, values, text)
        param_grads, value_grads, text_grads = pull(cotangent)
        totals = jax.tree.map(lambda left, right: left + right, totals, param_grads)
        return (totals, (result, value_grads, text_grads))
    zero_grads = tuple((jnp.zeros_like(item) for item in params))
    totals, (results, value_grads, text_grads) = lax.scan(clip_step, zero_grads, (clip_rows, text_states, clip_grads))
    return (results.reshape(TOKENS, D), value_grads.reshape(TOKENS, D), text_grads, totals[0], totals[1], totals[2], totals[3], totals[4], totals[5], totals[6], totals[7], totals[8])
```

```python
import functools
import math

import jax
import jax.numpy as jnp
from jax import lax
from jax.experimental import pallas as pl
from jax.experimental.pallas import tpu as pltpu
from jax.sharding import Mesh
from jax.sharding import PartitionSpec as P

HEAD_DIM = 64


EPSILON = 1e-05
MASKED = -1e30


def normalize(values, gain, shift):
    centre = jnp.mean(values, axis=1, keepdims=True)
    centred = values - centre
    spread = jnp.mean(centred * centred, axis=1, keepdims=True)
    return centred * lax.rsqrt(spread + EPSILON) * gain + shift


def activate(values):
    return jax.nn.gelu(values, approximate=False)


def gather_rows(local_rows):
    return lax.all_gather(local_rows, "tensor", axis=0, tiled=True)


def project_rows(operand, weight, leading):
    if leading:
        pattern = "tkc,cd->td"
    else:
        pattern = "tkc,dkc->td"
    return lax.psum_scatter(
        jnp.einsum(pattern, operand, weight, preferred_element_type=jnp.float32),
        "tensor",
        scatter_dimension=0,
        tiled=True,
    )


def score_block(query_block, keys, offset, causal):
    scale_factor = 1.0 / math.sqrt(query_block.shape[2])
    scores = (
        jnp.einsum("bhe,khe->hbk", query_block, keys, preferred_element_type=jnp.float32)
        * scale_factor
    )
    if causal:
        query_pos = offset + lax.broadcasted_iota(
            jnp.int32, (query_block.shape[0], keys.shape[0]), 0
        )
        key_pos = lax.broadcasted_iota(jnp.int32, (query_block.shape[0], keys.shape[0]), 1)
        scores = jnp.where((key_pos <= query_pos)[None], scores, MASKED)
    return scores


def attend(queries, keys, values, causal):
    length = queries.shape[0]
    block = min(512, length)

    def one_block(number):
        offset = number * block
        query_block = lax.dynamic_slice_in_dim(queries, offset, block, 0)
        scores = score_block(query_block, keys, offset, causal)
        highest = jnp.max(scores, axis=2, keepdims=True)
        raised = jnp.exp(scores - highest)
        totals = jnp.sum(raised, axis=2, keepdims=True)
        weights = (raised / totals).astype(jnp.bfloat16)
        mixed = jnp.einsum("hbk,khe->bhe", weights, values, preferred_element_type=jnp.float32)
        return (mixed.astype(jnp.bfloat16), (highest + jnp.log(totals))[:, :, 0])

    mixed, log_totals = lax.map(one_block, jnp.arange(length // block, dtype=jnp.int32))
    return (mixed.reshape(queries.shape), log_totals)


def attend_back(queries, keys, values, log_totals, out_grads, causal):
    length = queries.shape[0]
    block = min(512, length)
    scale_factor = 1.0 / math.sqrt(queries.shape[2])

    def one_block(carried, number):
        key_grads, value_grads = carried
        offset = number * block
        query_block = lax.dynamic_slice_in_dim(queries, offset, block, 0)
        grad_block = lax.dynamic_slice_in_dim(out_grads, offset, block, 0)
        scores = score_block(query_block, keys, offset, causal)
        probs = jnp.exp(scores - log_totals[number][:, :, None])
        prob_grads = jnp.einsum(
            "bhe,khe->hbk", grad_block, values, preferred_element_type=jnp.float32
        )
        centre = jnp.sum(probs * prob_grads, axis=2, keepdims=True)
        score_grads = (probs * (prob_grads - centre)).astype(jnp.bfloat16)
        query_grads = (
            jnp.einsum("hbk,khe->bhe", score_grads, keys, preferred_element_type=jnp.float32)
            * scale_factor
        )
        key_grads = (
            key_grads
            + jnp.einsum(
                "hbk,bhe->khe", score_grads, query_block, preferred_element_type=jnp.float32
            )
            * scale_factor
        )
        value_grads = value_grads + jnp.einsum(
            "hbk,bhe->khe",
            probs.astype(jnp.bfloat16),
            grad_block,
            preferred_element_type=jnp.float32,
        )
        return ((key_grads, value_grads), query_grads)

    empty = jnp.zeros(keys.shape, jnp.float32)
    (key_grads, value_grads), query_grads = lax.scan(
        one_block, (empty, empty), jnp.arange(length // block, dtype=jnp.int32)
    )
    return (query_grads.reshape(queries.shape), key_grads, value_grads)


def on_device(
    states,
    text_states,
    norm_gains,
    norm_biases,
    self_qkv,
    self_out,
    cross_query,
    cross_kv,
    cross_out,
    mlp_up,
    mlp_down,
    out_grad,
):
    lane_count = self_qkv.shape[2]
    head_count = lane_count // HEAD_DIM
    fetched = (
        lax.all_gather(norm_gains.astype(jnp.bfloat16), "dp", axis=1, tiled=True),
        lax.all_gather(norm_biases.astype(jnp.bfloat16), "dp", axis=1, tiled=True),
        lax.all_gather(self_qkv.astype(jnp.bfloat16), "dp", axis=0, tiled=True),
        lax.all_gather(self_out.astype(jnp.bfloat16), "dp", axis=1, tiled=True),
        lax.all_gather(cross_query.astype(jnp.bfloat16), "dp", axis=0, tiled=True),
        lax.all_gather(cross_kv.astype(jnp.bfloat16), "dp", axis=0, tiled=True),
        lax.all_gather(cross_out.astype(jnp.bfloat16), "dp", axis=1, tiled=True),
        lax.all_gather(mlp_up.astype(jnp.bfloat16), "dp", axis=0, tiled=True),
        lax.all_gather(mlp_down.astype(jnp.bfloat16), "dp", axis=1, tiled=True),
    )
    gains_low, biases_low, w_qkv, w_self_out, w_query, w_kv, w_cross_out, w_up, w_down = fetched
    gains = gains_low.astype(jnp.float32)
    biases = biases_low.astype(jnp.float32)

    def split_heads(block):
        return block.reshape(block.shape[0], head_count, HEAD_DIM)

    def as_rows(block):
        return block.reshape(block.shape[0], 1, block.shape[-1])

    def as_columns(weight):
        return weight.reshape(weight.shape[0], 1, weight.shape[1])

    def norm_back(values, which, grads):
        _, pull = jax.vjp(normalize, values, gains[which], biases[which])
        return pull(grads)

    normed_one = gather_rows(normalize(states, gains[0], biases[0]).astype(jnp.bfloat16))
    triple = jnp.einsum(
        "td,dkc->tkc", normed_one, w_qkv, preferred_element_type=jnp.float32
    ).astype(jnp.bfloat16)
    self_queries = split_heads(triple[:, 0])
    self_keys = split_heads(triple[:, 1])
    self_values = split_heads(triple[:, 2])
    self_mixed, self_totals = attend(self_queries, self_keys, self_values, True)
    self_flat = self_mixed.reshape(-1, lane_count)
    after_self = states + project_rows(as_rows(self_flat), w_self_out, True)
    normed_two = gather_rows(normalize(after_self, gains[1], biases[1]).astype(jnp.bfloat16))
    cross_queries = jnp.dot(normed_two, w_query, preferred_element_type=jnp.float32).astype(
        jnp.bfloat16
    )
    text_low = text_states[0].astype(jnp.bfloat16)
    text_pair = jnp.einsum(
        "td,dkc->tkc", text_low, w_kv, preferred_element_type=jnp.float32
    ).astype(jnp.bfloat16)
    text_keys = split_heads(text_pair[:, 0])
    text_values = split_heads(text_pair[:, 1])
    cross_mixed, cross_totals = attend(split_heads(cross_queries), text_keys, text_values, False)
    cross_flat = cross_mixed.reshape(-1, lane_count)
    after_cross = after_self + project_rows(as_rows(cross_flat), w_cross_out, True)
    normed_three = gather_rows(normalize(after_cross, gains[2], biases[2]).astype(jnp.bfloat16))
    hidden_pre = jnp.dot(normed_three, w_up, preferred_element_type=jnp.float32)
    hidden = activate(hidden_pre).astype(jnp.bfloat16)
    layer_out = after_cross + project_rows(as_rows(hidden), w_down, True)
    branch_grads = gather_rows(out_grad.astype(jnp.bfloat16))
    down_grad = jnp.einsum("tf,td->fd", hidden, branch_grads, preferred_element_type=jnp.float32)
    hidden_grad = jnp.einsum("td,fd->tf", branch_grads, w_down, preferred_element_type=jnp.float32)
    _, pull_act = jax.vjp(activate, hidden_pre)
    pre_grad = pull_act(hidden_grad)[0].astype(jnp.bfloat16)
    up_grad = jnp.einsum("td,tf->df", normed_three, pre_grad, preferred_element_type=jnp.float32)
    back_three = project_rows(as_rows(pre_grad), as_columns(w_up), False)
    rows_three, gain_three, shift_three = norm_back(after_cross, 2, back_three)
    cross_rows_grad = out_grad + rows_three
    cross_grads = gather_rows(cross_rows_grad.astype(jnp.bfloat16))
    cross_out_grad = jnp.einsum(
        "tc,td->cd", cross_flat, cross_grads, preferred_element_type=jnp.float32
    )
    cross_mixed_grad = jnp.einsum(
        "td,cd->tc", cross_grads, w_cross_out, preferred_element_type=jnp.float32
    ).astype(jnp.bfloat16)
    query_grad, text_key_grad, text_value_grad = attend_back(
        split_heads(cross_queries),
        text_keys,
        text_values,
        cross_totals,
        split_heads(cross_mixed_grad),
        False,
    )
    query_grad = query_grad.reshape(-1, lane_count).astype(jnp.bfloat16)
    pair_grad = jnp.stack(
        [text_key_grad.reshape(-1, lane_count), text_value_grad.reshape(-1, lane_count)], axis=1
    ).astype(jnp.bfloat16)
    query_weight_grad = jnp.einsum(
        "td,tc->dc", normed_two, query_grad, preferred_element_type=jnp.float32
    )
    kv_weight_grad = jnp.einsum(
        "td,tkc->dkc", text_low, pair_grad, preferred_element_type=jnp.float32
    )
    text_grad_part = jnp.einsum("tkc,dkc->td", pair_grad, w_kv, preferred_element_type=jnp.float32)
    back_two = project_rows(as_rows(query_grad), as_columns(w_query), False)
    rows_two, gain_two, shift_two = norm_back(after_self, 1, back_two)
    self_rows_grad = cross_rows_grad + rows_two
    self_grads = gather_rows(self_rows_grad.astype(jnp.bfloat16))
    self_out_grad = jnp.einsum(
        "tc,td->cd", self_flat, self_grads, preferred_element_type=jnp.float32
    )
    self_mixed_grad = jnp.einsum(
        "td,cd->tc", self_grads, w_self_out, preferred_element_type=jnp.float32
    ).astype(jnp.bfloat16)
    self_query_grad, self_key_grad, self_value_grad = attend_back(
        self_queries, self_keys, self_values, self_totals, split_heads(self_mixed_grad), True
    )
    triple_grad = jnp.stack(
        [
            self_query_grad.reshape(-1, lane_count),
            self_key_grad.reshape(-1, lane_count),
            self_value_grad.reshape(-1, lane_count),
        ],
        axis=1,
    ).astype(jnp.bfloat16)
    qkv_weight_grad = jnp.einsum(
        "td,tkc->dkc", normed_one, triple_grad, preferred_element_type=jnp.float32
    )
    back_one = project_rows(triple_grad, w_qkv, False)
    rows_one, gain_one, shift_one = norm_back(states, 0, back_one)
    states_grad = self_rows_grad + rows_one
    gain_parts = jnp.stack([gain_one, gain_two, gain_three])
    shift_parts = jnp.stack([shift_one, shift_two, shift_three])
    text_total, gain_total, shift_total = lax.psum(
        (text_grad_part, gain_parts, shift_parts), "tensor"
    )
    summed = (
        lax.psum_scatter(gain_total, "dp", scatter_dimension=1, tiled=True),
        lax.psum_scatter(shift_total, "dp", scatter_dimension=1, tiled=True),
        lax.psum_scatter(qkv_weight_grad, "dp", scatter_dimension=0, tiled=True),
        lax.psum_scatter(self_out_grad, "dp", scatter_dimension=1, tiled=True),
        lax.psum_scatter(query_weight_grad, "dp", scatter_dimension=0, tiled=True),
        lax.psum_scatter(kv_weight_grad, "dp", scatter_dimension=0, tiled=True),
        lax.psum_scatter(cross_out_grad, "dp", scatter_dimension=1, tiled=True),
        lax.psum_scatter(up_grad, "dp", scatter_dimension=0, tiled=True),
        lax.psum_scatter(down_grad, "dp", scatter_dimension=1, tiled=True),
    )
    (
        gain_sum,
        shift_sum,
        qkv_sum,
        self_out_sum,
        query_sum,
        kv_sum,
        cross_out_sum,
        up_sum,
        down_sum,
    ) = summed
    return (
        layer_out,
        states_grad,
        text_total[None],
        gain_sum,
        shift_sum,
        qkv_sum,
        self_out_sum,
        query_sum,
        kv_sum,
        cross_out_sum,
        up_sum,
        down_sum,
    )


PAIR = 2 * HEAD_DIM
ROWS_STEP = 512
LOG2E = 1.4426950408889634
VMEM_BYTES = 60 * 1024 * 1024


def dot_last(left, right):
    return lax.dot_general(left, right, (((1,), (1,)), ((), ())), preferred_element_type=jnp.float32)


def dot_first(left, right):
    return lax.dot_general(left, right, (((0,), (0,)), ((), ())), preferred_element_type=jnp.float32)


def key_spans(step, block, key_count, causal):
    if not causal:
        return [(0, key_count, False)]
    spans = [(0, step * block, False)] if step else []
    return spans + [(step * block, block, True)]


def causal_keep(block):
    key_pos = lax.broadcasted_iota(jnp.int32, (block, block), 0)
    query_pos = lax.broadcasted_iota(jnp.int32, (block, block), 1)
    return key_pos <= query_pos


def head_lanes(head):
    lanes = lax.broadcasted_iota(jnp.int32, (1, PAIR), 1)
    return (lanes >= HEAD_DIM) == (head == 1)


def attend_kernel(causal, block, q_ref, k_ref, v_ref, out_ref, log_ref, total_ref):
    length, key_count = q_ref.shape[0], k_ref.shape[0]
    scale = LOG2E / math.sqrt(HEAD_DIM)

    def one_head(head, carry):
        keep = head_lanes(head)
        mask = keep.astype(jnp.float32).astype(jnp.bfloat16)
        for step in range(length // block):
            rows = pl.ds(step * block, block)
            queries = q_ref[rows, :] * mask
            scores = []
            for start, count, diagonal in key_spans(step, block, key_count, causal):
                part = dot_last(k_ref[pl.ds(start, count), :], queries)
                if diagonal:
                    part = jnp.where(causal_keep(block), part, MASKED)
                scores.append(part)
            highest = jnp.max(scores[0], axis=0, keepdims=True)
            for part in scores[1:]:
                highest = jnp.maximum(highest, jnp.max(part, axis=0, keepdims=True))
            total, mixed = None, None
            for part, (start, count, _) in zip(scores, key_spans(step, block, key_count, causal)):
                raised = jnp.exp2((part - highest) * scale)
                summed = jnp.sum(raised, axis=0, keepdims=True)
                product = dot_first(v_ref[pl.ds(start, count), :], raised.astype(jnp.bfloat16))
                total = summed if total is None else total + summed
                mixed = product if mixed is None else mixed + product
            total_ref[rows, :] = jnp.where(keep, (mixed / total).T, total_ref[rows, :])
            log_ref[0, pl.ds(head, 1), rows] = highest * scale + jnp.log2(total)
        return carry

    lax.fori_loop(0, 2, one_head, 0)
    out_ref[...] = total_ref[...].astype(jnp.bfloat16)


def attend_back_body(
    causal, block, q_ref, k_ref, v_ref, grad_ref, log_ref, dq_ref, dk_ref, dv_ref
):
    length, key_count = q_ref.shape[0], k_ref.shape[0]
    scale = 1.0 / math.sqrt(HEAD_DIM)
    dk_ref[...] = jnp.zeros_like(dk_ref)
    dv_ref[...] = jnp.zeros_like(dv_ref)

    def one_head(head, carry):
        keep = head_lanes(head)
        mask = keep.astype(jnp.float32).astype(jnp.bfloat16)
        for step in range(length // block):
            rows = pl.ds(step * block, block)
            queries = q_ref[rows, :] * mask
            grads = grad_ref[rows, :] * mask
            logs = log_ref[0, pl.ds(head, 1), rows]
            spans = key_spans(step, block, key_count, causal)
            held, centre = [], None
            for start, count, diagonal in spans:
                keys = pl.ds(start, count)
                probs = jnp.exp2(dot_last(k_ref[keys, :], queries) * (scale * LOG2E) - logs)
                if diagonal:
                    probs = jnp.where(causal_keep(block), probs, 0.0)
                dv_ref[keys, :] += jnp.dot(
                    probs.astype(jnp.bfloat16), grads, preferred_element_type=jnp.float32
                )
                prob_grads = dot_last(v_ref[keys, :], grads)
                summed = jnp.sum(probs * prob_grads, axis=0, keepdims=True)
                centre = summed if centre is None else centre + summed
                held.append((probs, prob_grads))
            mixed = None
            for (probs, prob_grads), (start, count, _) in zip(held, spans):
                keys = pl.ds(start, count)
                score_grads = (probs * (prob_grads - centre)).astype(jnp.bfloat16)
                dk_ref[keys, :] += jnp.dot(
                    score_grads, queries, preferred_element_type=jnp.float32
                )
                product = dot_first(k_ref[keys, :], score_grads)
                mixed = product if mixed is None else mixed + product
            dq_ref[rows, :] = jnp.where(keep, mixed.T, dq_ref[rows, :])
        return carry

    lax.fori_loop(0, 2, one_head, 0)


def self_back_kernel(
    block, q_ref, k_ref, v_ref, grad_ref, log_ref, out_ref, dq_ref, dk_ref, dv_ref
):
    scale = 1.0 / math.sqrt(HEAD_DIM)
    part = pl.program_id(1)

    @pl.when(part == 0)
    def _():
        attend_back_body(
            True, block, q_ref, k_ref, v_ref, grad_ref, log_ref, dq_ref, dk_ref, dv_ref
        )
        out_ref[...] = (dq_ref[...] * scale).astype(jnp.bfloat16)

    @pl.when(part == 1)
    def _():
        out_ref[...] = (dk_ref[...] * scale).astype(jnp.bfloat16)

    @pl.when(part == 2)
    def _():
        out_ref[...] = dv_ref[...].astype(jnp.bfloat16)


def cross_back_kernel(
    block,
    q_ref,
    k_ref,
    v_ref,
    grad_ref,
    log_ref,
    query_ref,
    key_ref,
    value_ref,
    dq_ref,
    dk_ref,
    dv_ref,
):
    scale = 1.0 / math.sqrt(HEAD_DIM)
    attend_back_body(
        False, block, q_ref, k_ref, v_ref, grad_ref, log_ref, dq_ref, dk_ref, dv_ref
    )
    query_ref[...] = (dq_ref[...] * scale).astype(jnp.bfloat16)
    key_ref[...] = (dk_ref[...] * scale).astype(jnp.bfloat16)
    value_ref[...] = dv_ref[...].astype(jnp.bfloat16)


def column_spec(rows, first):
    return pl.BlockSpec((rows, PAIR), lambda pair, *rest: (0, first + pair))


def log_spec(rows):
    return pl.BlockSpec((1, 2, rows), lambda pair, *rest: (pair, 0, 0))


def attention_cost(length, key_count, lanes, products):
    return pl.CostEstimate(
        flops=2 * products * length * key_count * lanes,
        transcendentals=length * key_count * lanes // HEAD_DIM,
        bytes_accessed=2 * products * (length + key_count) * lanes,
    )


def fused_attend(queries, keys, first_key, first_value, lanes, causal):
    length, key_count = queries.shape[0], keys.shape[0]
    pairs = lanes // PAIR
    block = min(ROWS_STEP, length)
    return pl.pallas_call(
        functools.partial(attend_kernel, causal, block),
        grid=(pairs,),
        in_specs=[
            column_spec(length, 0),
            column_spec(key_count, first_key),
            column_spec(key_count, first_value),
        ],
        out_specs=[column_spec(length, 0), log_spec(length)],
        out_shape=[
            jax.ShapeDtypeStruct((length, lanes), jnp.bfloat16),
            jax.ShapeDtypeStruct((pairs, 2, length), jnp.float32),
        ],
        scratch_shapes=[pltpu.VMEM((length, PAIR), jnp.float32)],
        compiler_params=pltpu.CompilerParams(vmem_limit_bytes=VMEM_BYTES),
        cost_estimate=attention_cost(length, key_count, lanes, 2),
        name="attend_self" if causal else "attend_cross",
    )(queries, keys, keys)


def accumulators(length, key_count):
    return [
        pltpu.VMEM((length, PAIR), jnp.float32),
        pltpu.VMEM((key_count, PAIR), jnp.float32),
        pltpu.VMEM((key_count, PAIR), jnp.float32),
    ]


def fused_self_back(triple, logs, grads):
    length, lanes = grads.shape
    pairs = lanes // PAIR
    return pl.pallas_call(
        functools.partial(self_back_kernel, min(ROWS_STEP, length)),
        grid=(pairs, 3),
        in_specs=[
            column_spec(length, 0),
            column_spec(length, pairs),
            column_spec(length, 2 * pairs),
            column_spec(length, 0),
            log_spec(length),
        ],
        out_specs=pl.BlockSpec((length, PAIR), lambda pair, part: (0, part * pairs + pair)),
        out_shape=jax.ShapeDtypeStruct((length, 3 * lanes), jnp.bfloat16),
        scratch_shapes=accumulators(length, length),
        compiler_params=pltpu.CompilerParams(vmem_limit_bytes=VMEM_BYTES),
        cost_estimate=attention_cost(length, length, lanes, 5),
        name="attend_self_back",
    )(triple, triple, triple, grads, logs)


def fused_cross_back(queries, text_pair, logs, grads):
    length, lanes = grads.shape
    key_count = text_pair.shape[0]
    pairs = lanes // PAIR
    return pl.pallas_call(
        functools.partial(cross_back_kernel, min(ROWS_STEP, length)),
        grid=(pairs,),
        in_specs=[
            column_spec(length, 0),
            column_spec(key_count, 0),
            column_spec(key_count, pairs),
            column_spec(length, 0),
            log_spec(length),
        ],
        out_specs=[column_spec(length, 0), column_spec(key_count, 0), column_spec(key_count, 0)],
        out_shape=[
            jax.ShapeDtypeStruct((length, lanes), jnp.bfloat16),
            jax.ShapeDtypeStruct((key_count, lanes), jnp.bfloat16),
            jax.ShapeDtypeStruct((key_count, lanes), jnp.bfloat16),
        ],
        scratch_shapes=accumulators(length, key_count),
        compiler_params=pltpu.CompilerParams(vmem_limit_bytes=VMEM_BYTES),
        cost_estimate=attention_cost(length, key_count, lanes, 5),
        name="attend_cross_back",
    )(queries, text_pair, text_pair, grads, logs)


SPREAD = ("site", "y")


def low(values):
    return values.astype(jnp.bfloat16)


def trade_corners(values):
    return lax.ppermute(values, ("core", "y"), [(0, 0), (1, 2), (2, 1), (3, 3)])


def to_mate(values):
    return lax.ppermute(values, "core", [(0, 1), (1, 0)])


def gather_pair(local_rows):
    other = to_mate(local_rows)
    first = lax.axis_index("core") == 0
    return jnp.concatenate(
        [jnp.where(first, local_rows, other), jnp.where(first, other, local_rows)], axis=0
    )


def scatter_pair(operand, product):
    rows = operand.shape[0] // 2
    core = lax.axis_index("core")
    theirs = low(product(lax.dynamic_slice_in_dim(operand, (1 - core) * rows, rows, 0)))
    received = to_mate(theirs)
    mine = product(lax.dynamic_slice_in_dim(operand, core * rows, rows, 0))
    return mine + received.astype(jnp.float32)


def fetch(shard):
    return lax.all_gather(trade_corners(shard), SPREAD, axis=0, tiled=True)


def share_grad(grad):
    summed = lax.psum_scatter(low(grad), SPREAD, scatter_dimension=0, tiled=True)
    return trade_corners(summed).astype(jnp.float32)


def on_pair(
    states,
    text_states,
    norm_gains,
    norm_biases,
    self_qkv,
    self_out,
    cross_query,
    cross_kv,
    cross_out,
    mlp_up,
    mlp_down,
    out_grad,
):
    depth, _, lanes = self_qkv.shape
    pairs = lanes // PAIR
    f32 = jnp.float32
    norms = lax.all_gather(
        low(jnp.concatenate([norm_gains, norm_biases], axis=0)), ("site", "core"), axis=1, tiled=True
    ).astype(f32)
    gains, biases = norms[:3], norms[3:]
    w_qkv = fetch(low(self_qkv).reshape(depth, 3 * lanes))
    w_self_out = fetch(low(self_out).T)
    w_kv = fetch(low(cross_kv).reshape(depth, 2 * lanes))
    w_query = fetch(low(cross_query))
    w_cross_out = fetch(low(cross_out).T)
    w_up = fetch(low(mlp_up))
    w_down = fetch(low(mlp_down).T)
    rows = trade_corners(states)
    text_low = trade_corners(low(text_states[0]))
    grad_rows = trade_corners(low(out_grad))

    def norm_back(values, which, grads):
        _, pull = jax.vjp(normalize, values, gains[which], biases[which])
        return pull(grads)

    def dot(left, right):
        return jnp.dot(left, right, preferred_element_type=f32)

    normed_one = gather_pair(low(normalize(rows, gains[0], biases[0])))
    triple = low(dot(normed_one, w_qkv))
    self_mixed, self_logs = fused_attend(triple, triple, pairs, 2 * pairs, lanes, True)
    after_self = rows + scatter_pair(self_mixed, lambda part: dot_last(part, w_self_out))
    normed_two = gather_pair(low(normalize(after_self, gains[1], biases[1])))
    queries = low(dot(normed_two, w_query))
    text_pair = low(dot(text_low, w_kv))
    cross_mixed, cross_logs = fused_attend(queries, text_pair, 0, pairs, lanes, False)
    after_cross = after_self + scatter_pair(cross_mixed, lambda part: dot_last(part, w_cross_out))
    normed_three = gather_pair(low(normalize(after_cross, gains[2], biases[2])))
    hidden_pre = dot(normed_three, w_up)
    hidden = low(activate(hidden_pre))
    layer_out = trade_corners(
        after_cross + scatter_pair(hidden, lambda part: dot_last(part, w_down))
    )
    branch_grads = gather_pair(grad_rows)
    down_grad = share_grad(dot_first(branch_grads, hidden)).T
    hidden_grad = dot(branch_grads, w_down)
    _, pull_act = jax.vjp(activate, hidden_pre)
    pre_grad = low(pull_act(hidden_grad)[0])
    up_grad = share_grad(dot_first(normed_three, pre_grad))
    back_three = scatter_pair(pre_grad, lambda part: dot_last(part, w_up))
    rows_three, gain_three, shift_three = norm_back(after_cross, 2, back_three)
    cross_rows_grad = grad_rows.astype(f32) + rows_three
    cross_grads = gather_pair(low(cross_rows_grad))
    cross_out_grad = share_grad(dot_first(cross_grads, cross_mixed)).T
    cross_mixed_grad = low(dot(cross_grads, w_cross_out))
    query_grad, key_grad, value_grad = fused_cross_back(
        queries, text_pair, cross_logs, cross_mixed_grad
    )
    pair_grad = jnp.concatenate([key_grad, value_grad], axis=1)
    query_weight_grad = share_grad(dot_first(normed_two, query_grad))
    kv_weight_grad = share_grad(dot_first(text_low, pair_grad)).reshape(depth, 2, lanes)
    text_part = dot_last(pair_grad, w_kv)
    text_grad = trade_corners(text_part + to_mate(text_part))
    back_two = scatter_pair(query_grad, lambda part: dot_last(part, w_query))
    rows_two, gain_two, shift_two = norm_back(after_self, 1, back_two)
    self_rows_grad = cross_rows_grad + rows_two
    self_grads = gather_pair(low(self_rows_grad))
    self_out_grad = share_grad(dot_first(self_grads, self_mixed)).T
    self_mixed_grad = low(dot(self_grads, w_self_out))
    triple_grad = fused_self_back(triple, self_logs, self_mixed_grad)
    qkv_grad = share_grad(dot_first(normed_one, triple_grad)).reshape(depth, 3, lanes)
    back_one = scatter_pair(triple_grad, lambda part: dot_last(part, w_qkv))
    rows_one, gain_one, shift_one = norm_back(rows, 0, back_one)
    states_grad = trade_corners(self_rows_grad + rows_one)
    norm_parts = jnp.stack([gain_one, gain_two, gain_three, shift_one, shift_two, shift_three])
    norm_total = lax.psum(norm_parts, ("site", "core", "y"))
    width = norm_gains.shape[1]
    place = lax.axis_index("site") * 2 + lax.axis_index("core")
    norm_own = lax.dynamic_slice_in_dim(norm_total, place * width, width, 1)
    return (
        layer_out,
        states_grad,
        text_grad[None],
        norm_own[:3],
        norm_own[3:],
        qkv_grad,
        self_out_grad,
        query_weight_grad,
        kv_weight_grad,
        cross_out_grad,
        up_grad,
        down_grad,
    )


def placements(dp, tensor):
    both = (*dp, *tensor)
    weights = [
        P(dp, None, tensor),
        P(tensor, dp),
        P(dp, tensor),
        P(dp, None, tensor),
        P(tensor, dp),
        P(dp, tensor),
        P(tensor, dp),
    ]
    shared = [P(dp, None, None), P(None, dp), P(None, dp)]
    taken = (P(both, None), *shared, *weights, P(both, None))
    given = (P(both, None), P(both, None), *shared, *weights)
    return taken, given


def solution(mesh):
    dp, tensor = mesh.shape["dp"], mesh.shape["tensor"]
    if tensor == 2 and dp % 2 == 0:
        body = on_pair
        mesh = Mesh(mesh.devices.reshape(dp // 2, 2, 2), ("site", "core", "y"))
        taken, given = placements(("site", "core"), ("y",))
    else:
        body = on_device
        taken, given = placements(("dp",), ("tensor",))
    return jax.shard_map(body, mesh=mesh, in_specs=taken, out_specs=given, check_vma=False)
```

```python
import functools
import math

import jax
import jax.numpy as jnp
from jax import lax
from jax.experimental import pallas as pl
from jax.experimental.pallas import tpu as pltpu
from jax.sharding import Mesh
from jax.sharding import PartitionSpec as P

HEAD_DIM = 64


EPSILON = 1e-05
MASKED = -1e30


def normalize(values, gain, shift):
    centre = jnp.mean(values, axis=1, keepdims=True)
    centred = values - centre
    spread = jnp.mean(centred * centred, axis=1, keepdims=True)
    return centred * lax.rsqrt(spread + EPSILON) * gain + shift


def activate(values):
    return jax.nn.gelu(values, approximate=False)


def gather_rows(local_rows):
    return lax.all_gather(local_rows, "tensor", axis=0, tiled=True)


def project_rows(operand, weight, leading):
    if leading:
        pattern = "tkc,cd->td"
    else:
        pattern = "tkc,dkc->td"
    return lax.psum_scatter(
        jnp.einsum(pattern, operand, weight, preferred_element_type=jnp.float32),
        "tensor",
        scatter_dimension=0,
        tiled=True,
    )


def score_block(query_block, keys, offset, causal):
    scale_factor = 1.0 / math.sqrt(query_block.shape[2])
    scores = (
        jnp.einsum("bhe,khe->hbk", query_block, keys, preferred_element_type=jnp.float32)
        * scale_factor
    )
    if causal:
        query_pos = offset + lax.broadcasted_iota(
            jnp.int32, (query_block.shape[0], keys.shape[0]), 0
        )
        key_pos = lax.broadcasted_iota(jnp.int32, (query_block.shape[0], keys.shape[0]), 1)
        scores = jnp.where((key_pos <= query_pos)[None], scores, MASKED)
    return scores


def attend(queries, keys, values, causal):
    length = queries.shape[0]
    block = min(512, length)

    def one_block(number):
        offset = number * block
        query_block = lax.dynamic_slice_in_dim(queries, offset, block, 0)
        scores = score_block(query_block, keys, offset, causal)
        highest = jnp.max(scores, axis=2, keepdims=True)
        raised = jnp.exp(scores - highest)
        totals = jnp.sum(raised, axis=2, keepdims=True)
        weights = (raised / totals).astype(jnp.bfloat16)
        mixed = jnp.einsum("hbk,khe->bhe", weights, values, preferred_element_type=jnp.float32)
        return (mixed.astype(jnp.bfloat16), (highest + jnp.log(totals))[:, :, 0])

    mixed, log_totals = lax.map(one_block, jnp.arange(length // block, dtype=jnp.int32))
    return (mixed.reshape(queries.shape), log_totals)


def attend_back(queries, keys, values, log_totals, out_grads, causal):
    length = queries.shape[0]
    block = min(512, length)
    scale_factor = 1.0 / math.sqrt(queries.shape[2])

    def one_block(carried, number):
        key_grads, value_grads = carried
        offset = number * block
        query_block = lax.dynamic_slice_in_dim(queries, offset, block, 0)
        grad_block = lax.dynamic_slice_in_dim(out_grads, offset, block, 0)
        scores = score_block(query_block, keys, offset, causal)
        probs = jnp.exp(scores - log_totals[number][:, :, None])
        prob_grads = jnp.einsum(
            "bhe,khe->hbk", grad_block, values, preferred_element_type=jnp.float32
        )
        centre = jnp.sum(probs * prob_grads, axis=2, keepdims=True)
        score_grads = (probs * (prob_grads - centre)).astype(jnp.bfloat16)
        query_grads = (
            jnp.einsum("hbk,khe->bhe", score_grads, keys, preferred_element_type=jnp.float32)
            * scale_factor
        )
        key_grads = (
            key_grads
            + jnp.einsum(
                "hbk,bhe->khe", score_grads, query_block, preferred_element_type=jnp.float32
            )
            * scale_factor
        )
        value_grads = value_grads + jnp.einsum(
            "hbk,bhe->khe",
            probs.astype(jnp.bfloat16),
            grad_block,
            preferred_element_type=jnp.float32,
        )
        return ((key_grads, value_grads), query_grads)

    empty = jnp.zeros(keys.shape, jnp.float32)
    (key_grads, value_grads), query_grads = lax.scan(
        one_block, (empty, empty), jnp.arange(length // block, dtype=jnp.int32)
    )
    return (query_grads.reshape(queries.shape), key_grads, value_grads)


def on_device(
    states,
    text_states,
    norm_gains,
    norm_biases,
    self_qkv,
    self_out,
    cross_query,
    cross_kv,
    cross_out,
    mlp_up,
    mlp_down,
    out_grad,
):
    lane_count = self_qkv.shape[2]
    head_count = lane_count // HEAD_DIM
    fetched = (
        lax.all_gather(norm_gains.astype(jnp.bfloat16), "dp", axis=1, tiled=True),
        lax.all_gather(norm_biases.astype(jnp.bfloat16), "dp", axis=1, tiled=True),
        lax.all_gather(self_qkv.astype(jnp.bfloat16), "dp", axis=0, tiled=True),
        lax.all_gather(self_out.astype(jnp.bfloat16), "dp", axis=1, tiled=True),
        lax.all_gather(cross_query.astype(jnp.bfloat16), "dp", axis=0, tiled=True),
        lax.all_gather(cross_kv.astype(jnp.bfloat16), "dp", axis=0, tiled=True),
        lax.all_gather(cross_out.astype(jnp.bfloat16), "dp", axis=1, tiled=True),
        lax.all_gather(mlp_up.astype(jnp.bfloat16), "dp", axis=0, tiled=True),
        lax.all_gather(mlp_down.astype(jnp.bfloat16), "dp", axis=1, tiled=True),
    )
    gains_low, biases_low, w_qkv, w_self_out, w_query, w_kv, w_cross_out, w_up, w_down = fetched
    gains = gains_low.astype(jnp.float32)
    biases = biases_low.astype(jnp.float32)

    def split_heads(block):
        return block.reshape(block.shape[0], head_count, HEAD_DIM)

    def as_rows(block):
        return block.reshape(block.shape[0], 1, block.shape[-1])

    def as_columns(weight):
        return weight.reshape(weight.shape[0], 1, weight.shape[1])

    def norm_back(values, which, grads):
        _, pull = jax.vjp(normalize, values, gains[which], biases[which])
        return pull(grads)

    normed_one = gather_rows(normalize(states, gains[0], biases[0]).astype(jnp.bfloat16))
    triple = jnp.einsum(
        "td,dkc->tkc", normed_one, w_qkv, preferred_element_type=jnp.float32
    ).astype(jnp.bfloat16)
    self_queries = split_heads(triple[:, 0])
    self_keys = split_heads(triple[:, 1])
    self_values = split_heads(triple[:, 2])
    self_mixed, self_totals = attend(self_queries, self_keys, self_values, True)
    self_flat = self_mixed.reshape(-1, lane_count)
    after_self = states + project_rows(as_rows(self_flat), w_self_out, True)
    normed_two = gather_rows(normalize(after_self, gains[1], biases[1]).astype(jnp.bfloat16))
    cross_queries = jnp.dot(normed_two, w_query, preferred_element_type=jnp.float32).astype(
        jnp.bfloat16
    )
    text_low = text_states[0].astype(jnp.bfloat16)
    text_pair = jnp.einsum(
        "td,dkc->tkc", text_low, w_kv, preferred_element_type=jnp.float32
    ).astype(jnp.bfloat16)
    text_keys = split_heads(text_pair[:, 0])
    text_values = split_heads(text_pair[:, 1])
    cross_mixed, cross_totals = attend(split_heads(cross_queries), text_keys, text_values, False)
    cross_flat = cross_mixed.reshape(-1, lane_count)
    after_cross = after_self + project_rows(as_rows(cross_flat), w_cross_out, True)
    normed_three = gather_rows(normalize(after_cross, gains[2], biases[2]).astype(jnp.bfloat16))
    hidden_pre = jnp.dot(normed_three, w_up, preferred_element_type=jnp.float32)
    hidden = activate(hidden_pre).astype(jnp.bfloat16)
    layer_out = after_cross + project_rows(as_rows(hidden), w_down, True)
    branch_grads = gather_rows(out_grad.astype(jnp.bfloat16))
    down_grad = jnp.einsum("tf,td->fd", hidden, branch_grads, preferred_element_type=jnp.float32)
    hidden_grad = jnp.einsum("td,fd->tf", branch_grads, w_down, preferred_element_type=jnp.float32)
    _, pull_act = jax.vjp(activate, hidden_pre)
    pre_grad = pull_act(hidden_grad)[0].astype(jnp.bfloat16)
    up_grad = jnp.einsum("td,tf->df", normed_three, pre_grad, preferred_element_type=jnp.float32)
    back_three = project_rows(as_rows(pre_grad), as_columns(w_up), False)
    rows_three, gain_three, shift_three = norm_back(after_cross, 2, back_three)
    cross_rows_grad = out_grad + rows_three
    cross_grads = gather_rows(cross_rows_grad.astype(jnp.bfloat16))
    cross_out_grad = jnp.einsum(
        "tc,td->cd", cross_flat, cross_grads, preferred_element_type=jnp.float32
    )
    cross_mixed_grad = jnp.einsum(
        "td,cd->tc", cross_grads, w_cross_out, preferred_element_type=jnp.float32
    ).astype(jnp.bfloat16)
    query_grad, text_key_grad, text_value_grad = attend_back(
        split_heads(cross_queries),
        text_keys,
        text_values,
        cross_totals,
        split_heads(cross_mixed_grad),
        False,
    )
    query_grad = query_grad.reshape(-1, lane_count).astype(jnp.bfloat16)
    pair_grad = jnp.stack(
        [text_key_grad.reshape(-1, lane_count), text_value_grad.reshape(-1, lane_count)], axis=1
    ).astype(jnp.bfloat16)
    query_weight_grad = jnp.einsum(
        "td,tc->dc", normed_two, query_grad, preferred_element_type=jnp.float32
    )
    kv_weight_grad = jnp.einsum(
        "td,tkc->dkc", text_low, pair_grad, preferred_element_type=jnp.float32
    )
    text_grad_part = jnp.einsum("tkc,dkc->td", pair_grad, w_kv, preferred_element_type=jnp.float32)
    back_two = project_rows(as_rows(query_grad), as_columns(w_query), False)
    rows_two, gain_two, shift_two = norm_back(after_self, 1, back_two)
    self_rows_grad = cross_rows_grad + rows_two
    self_grads = gather_rows(self_rows_grad.astype(jnp.bfloat16))
    self_out_grad = jnp.einsum(
        "tc,td->cd", self_flat, self_grads, preferred_element_type=jnp.float32
    )
    self_mixed_grad = jnp.einsum(
        "td,cd->tc", self_grads, w_self_out, preferred_element_type=jnp.float32
    ).astype(jnp.bfloat16)
    self_query_grad, self_key_grad, self_value_grad = attend_back(
        self_queries, self_keys, self_values, self_totals, split_heads(self_mixed_grad), True
    )
    triple_grad = jnp.stack(
        [
            self_query_grad.reshape(-1, lane_count),
            self_key_grad.reshape(-1, lane_count),
            self_value_grad.reshape(-1, lane_count),
        ],
        axis=1,
    ).astype(jnp.bfloat16)
    qkv_weight_grad = jnp.einsum(
        "td,tkc->dkc", normed_one, triple_grad, preferred_element_type=jnp.float32
    )
    back_one = project_rows(triple_grad, w_qkv, False)
    rows_one, gain_one, shift_one = norm_back(states, 0, back_one)
    states_grad = self_rows_grad + rows_one
    gain_parts = jnp.stack([gain_one, gain_two, gain_three])
    shift_parts = jnp.stack([shift_one, shift_two, shift_three])
    text_total, gain_total, shift_total = lax.psum(
        (text_grad_part, gain_parts, shift_parts), "tensor"
    )
    summed = (
        lax.psum_scatter(gain_total, "dp", scatter_dimension=1, tiled=True),
        lax.psum_scatter(shift_total, "dp", scatter_dimension=1, tiled=True),
        lax.psum_scatter(qkv_weight_grad, "dp", scatter_dimension=0, tiled=True),
        lax.psum_scatter(self_out_grad, "dp", scatter_dimension=1, tiled=True),
        lax.psum_scatter(query_weight_grad, "dp", scatter_dimension=0, tiled=True),
        lax.psum_scatter(kv_weight_grad, "dp", scatter_dimension=0, tiled=True),
        lax.psum_scatter(cross_out_grad, "dp", scatter_dimension=1, tiled=True),
        lax.psum_scatter(up_grad, "dp", scatter_dimension=0, tiled=True),
        lax.psum_scatter(down_grad, "dp", scatter_dimension=1, tiled=True),
    )
    (
        gain_sum,
        shift_sum,
        qkv_sum,
        self_out_sum,
        query_sum,
        kv_sum,
        cross_out_sum,
        up_sum,
        down_sum,
    ) = summed
    return (
        layer_out,
        states_grad,
        text_total[None],
        gain_sum,
        shift_sum,
        qkv_sum,
        self_out_sum,
        query_sum,
        kv_sum,
        cross_out_sum,
        up_sum,
        down_sum,
    )


PAIR = 2 * HEAD_DIM
ROWS_STEP = 512
LOG2E = 1.4426950408889634
VMEM_BYTES = 60 * 1024 * 1024


def dot_last(left, right):
    return lax.dot_general(left, right, (((1,), (1,)), ((), ())), preferred_element_type=jnp.float32)


def dot_first(left, right):
    return lax.dot_general(left, right, (((0,), (0,)), ((), ())), preferred_element_type=jnp.float32)


def key_spans(step, block, key_count, causal):
    if not causal:
        return [(0, key_count, False)]
    spans = [(0, step * block, False)] if step else []
    return spans + [(step * block, block, True)]


def causal_keep(block):
    key_pos = lax.broadcasted_iota(jnp.int32, (block, block), 0)
    query_pos = lax.broadcasted_iota(jnp.int32, (block, block), 1)
    return key_pos <= query_pos


def head_lanes(head):
    lanes = lax.broadcasted_iota(jnp.int32, (1, PAIR), 1)
    return (lanes >= HEAD_DIM) == (head == 1)


def attend_kernel(causal, block, q_ref, k_ref, v_ref, out_ref, log_ref, total_ref):
    length, key_count = q_ref.shape[0], k_ref.shape[0]
    scale = LOG2E / math.sqrt(HEAD_DIM)

    def one_head(head, carry):
        keep = head_lanes(head)
        mask = keep.astype(jnp.float32).astype(jnp.bfloat16)
        for step in range(length // block):
            rows = pl.ds(step * block, block)
            queries = q_ref[rows, :] * mask
            scores = []
            for start, count, diagonal in key_spans(step, block, key_count, causal):
                part = dot_last(k_ref[pl.ds(start, count), :], queries)
                if diagonal:
                    part = jnp.where(causal_keep(block), part, MASKED)
                scores.append(part)
            highest = jnp.max(scores[0], axis=0, keepdims=True)
            for part in scores[1:]:
                highest = jnp.maximum(highest, jnp.max(part, axis=0, keepdims=True))
            total, mixed = None, None
            for part, (start, count, _) in zip(scores, key_spans(step, block, key_count, causal)):
                raised = jnp.exp2((part - highest) * scale)
                summed = jnp.sum(raised, axis=0, keepdims=True)
                product = dot_first(v_ref[pl.ds(start, count), :], raised.astype(jnp.bfloat16))
                total = summed if total is None else total + summed
                mixed = product if mixed is None else mixed + product
            total_ref[rows, :] = jnp.where(keep, (mixed / total).T, total_ref[rows, :])
            log_ref[0, pl.ds(head, 1), rows] = highest * scale + jnp.log2(total)
        return carry

    lax.fori_loop(0, 2, one_head, 0)
    out_ref[...] = total_ref[...].astype(jnp.bfloat16)


def attend_back_body(
    causal, block, q_ref, k_ref, v_ref, grad_ref, log_ref, dq_ref, dk_ref, dv_ref
):
    length, key_count = q_ref.shape[0], k_ref.shape[0]
    scale = 1.0 / math.sqrt(HEAD_DIM)
    dk_ref[...] = jnp.zeros_like(dk_ref)
    dv_ref[...] = jnp.zeros_like(dv_ref)

    def one_head(head, carry):
        keep = head_lanes(head)
        mask = keep.astype(jnp.float32).astype(jnp.bfloat16)
        for step in range(length // block):
            rows = pl.ds(step * block, block)
            queries = q_ref[rows, :] * mask
            grads = grad_ref[rows, :] * mask
            logs = log_ref[0, pl.ds(head, 1), rows]
            spans = key_spans(step, block, key_count, causal)
            held, centre = [], None
            for start, count, diagonal in spans:
                keys = pl.ds(start, count)
                probs = jnp.exp2(dot_last(k_ref[keys, :], queries) * (scale * LOG2E) - logs)
                if diagonal:
                    probs = jnp.where(causal_keep(block), probs, 0.0)
                dv_ref[keys, :] += jnp.dot(
                    probs.astype(jnp.bfloat16), grads, preferred_element_type=jnp.float32
                )
                prob_grads = dot_last(v_ref[keys, :], grads)
                summed = jnp.sum(probs * prob_grads, axis=0, keepdims=True)
                centre = summed if centre is None else centre + summed
                held.append((probs, prob_grads))
            mixed = None
            for (probs, prob_grads), (start, count, _) in zip(held, spans):
                keys = pl.ds(start, count)
                score_grads = (probs * (prob_grads - centre)).astype(jnp.bfloat16)
                dk_ref[keys, :] += jnp.dot(
                    score_grads, queries, preferred_element_type=jnp.float32
                )
                product = dot_first(k_ref[keys, :], score_grads)
                mixed = product if mixed is None else mixed + product
            dq_ref[rows, :] = jnp.where(keep, mixed.T, dq_ref[rows, :])
        return carry

    lax.fori_loop(0, 2, one_head, 0)


def self_back_kernel(
    block, q_ref, k_ref, v_ref, grad_ref, log_ref, out_ref, dq_ref, dk_ref, dv_ref
):
    scale = 1.0 / math.sqrt(HEAD_DIM)
    part = pl.program_id(1)

    @pl.when(part == 0)
    def _():
        attend_back_body(
            True, block, q_ref, k_ref, v_ref, grad_ref, log_ref, dq_ref, dk_ref, dv_ref
        )
        out_ref[...] = (dq_ref[...] * scale).astype(jnp.bfloat16)

    @pl.when(part == 1)
    def _():
        out_ref[...] = (dk_ref[...] * scale).astype(jnp.bfloat16)

    @pl.when(part == 2)
    def _():
        out_ref[...] = dv_ref[...].astype(jnp.bfloat16)


def cross_back_kernel(
    block,
    q_ref,
    k_ref,
    v_ref,
    grad_ref,
    log_ref,
    query_ref,
    key_ref,
    value_ref,
    dq_ref,
    dk_ref,
    dv_ref,
):
    scale = 1.0 / math.sqrt(HEAD_DIM)
    attend_back_body(
        False, block, q_ref, k_ref, v_ref, grad_ref, log_ref, dq_ref, dk_ref, dv_ref
    )
    query_ref[...] = (dq_ref[...] * scale).astype(jnp.bfloat16)
    key_ref[...] = (dk_ref[...] * scale).astype(jnp.bfloat16)
    value_ref[...] = dv_ref[...].astype(jnp.bfloat16)


def column_spec(rows, first):
    return pl.BlockSpec((rows, PAIR), lambda pair, *rest: (0, first + pair))


def log_spec(rows):
    return pl.BlockSpec((1, 2, rows), lambda pair, *rest: (pair, 0, 0))


def attention_cost(length, key_count, lanes, products):
    return pl.CostEstimate(
        flops=2 * products * length * key_count * lanes,
        transcendentals=length * key_count * lanes // HEAD_DIM,
        bytes_accessed=2 * products * (length + key_count) * lanes,
    )


def fused_attend(queries, keys, first_key, first_value, lanes, causal):
    length, key_count = queries.shape[0], keys.shape[0]
    pairs = lanes // PAIR
    block = min(ROWS_STEP, length)
    return pl.pallas_call(
        functools.partial(attend_kernel, causal, block),
        grid=(pairs,),
        in_specs=[
            column_spec(length, 0),
            column_spec(key_count, first_key),
            column_spec(key_count, first_value),
        ],
        out_specs=[column_spec(length, 0), log_spec(length)],
        out_shape=[
            jax.ShapeDtypeStruct((length, lanes), jnp.bfloat16),
            jax.ShapeDtypeStruct((pairs, 2, length), jnp.float32),
        ],
        scratch_shapes=[pltpu.VMEM((length, PAIR), jnp.float32)],
        compiler_params=pltpu.CompilerParams(vmem_limit_bytes=VMEM_BYTES),
        cost_estimate=attention_cost(length, key_count, lanes, 2),
        name="attend_self" if causal else "attend_cross",
    )(queries, keys, keys)


def accumulators(length, key_count):
    return [
        pltpu.VMEM((length, PAIR), jnp.float32),
        pltpu.VMEM((key_count, PAIR), jnp.float32),
        pltpu.VMEM((key_count, PAIR), jnp.float32),
    ]


def fused_self_back(triple, logs, grads):
    length, lanes = grads.shape
    pairs = lanes // PAIR
    return pl.pallas_call(
        functools.partial(self_back_kernel, min(ROWS_STEP, length)),
        grid=(pairs, 3),
        in_specs=[
            column_spec(length, 0),
            column_spec(length, pairs),
            column_spec(length, 2 * pairs),
            column_spec(length, 0),
            log_spec(length),
        ],
        out_specs=pl.BlockSpec((length, PAIR), lambda pair, part: (0, part * pairs + pair)),
        out_shape=jax.ShapeDtypeStruct((length, 3 * lanes), jnp.bfloat16),
        scratch_shapes=accumulators(length, length),
        compiler_params=pltpu.CompilerParams(vmem_limit_bytes=VMEM_BYTES),
        cost_estimate=attention_cost(length, length, lanes, 5),
        name="attend_self_back",
    )(triple, triple, triple, grads, logs)


def fused_cross_back(queries, text_pair, logs, grads):
    length, lanes = grads.shape
    key_count = text_pair.shape[0]
    pairs = lanes // PAIR
    return pl.pallas_call(
        functools.partial(cross_back_kernel, min(ROWS_STEP, length)),
        grid=(pairs,),
        in_specs=[
            column_spec(length, 0),
            column_spec(key_count, 0),
            column_spec(key_count, pairs),
            column_spec(length, 0),
            log_spec(length),
        ],
        out_specs=[column_spec(length, 0), column_spec(key_count, 0), column_spec(key_count, 0)],
        out_shape=[
            jax.ShapeDtypeStruct((length, lanes), jnp.bfloat16),
            jax.ShapeDtypeStruct((key_count, lanes), jnp.bfloat16),
            jax.ShapeDtypeStruct((key_count, lanes), jnp.bfloat16),
        ],
        scratch_shapes=accumulators(length, key_count),
        compiler_params=pltpu.CompilerParams(vmem_limit_bytes=VMEM_BYTES),
        cost_estimate=attention_cost(length, key_count, lanes, 5),
        name="attend_cross_back",
    )(queries, text_pair, text_pair, grads, logs)


def low(values):
    return values.astype(jnp.bfloat16)


def at_corner():
    return lax.axis_index("core") != lax.axis_index("y")


def trade_corners(values):
    received = lax.ppermute(values, ("core", "y"), [(1, 2), (2, 1)])
    return jnp.where(at_corner(), received, values)


def to_mate(values, axis="core"):
    return lax.ppermute(values, axis, [(0, 1), (1, 0)])


def gather_pair(local_rows):
    other = to_mate(local_rows)
    first = lax.axis_index("core") == 0
    return jnp.concatenate(
        [jnp.where(first, local_rows, other), jnp.where(first, other, local_rows)], axis=0
    )


def scatter_pair(operand, product):
    rows = operand.shape[0] // 2
    core = lax.axis_index("core")
    theirs = low(product(lax.dynamic_slice_in_dim(operand, (1 - core) * rows, rows, 0)))
    received = to_mate(theirs)
    mine = product(lax.dynamic_slice_in_dim(operand, core * rows, rows, 0))
    return mine + received.astype(jnp.float32)


ORDERS = (("x", "y"), ("y", "x"))


def fetch(shard):
    line = lax.all_gather(shard, "z", axis=0)
    count, rows, columns = line.shape
    width = columns // 2
    whole = jnp.broadcast_to(line[:, None, None], (count, 2, 2, rows, columns))
    for start, order in zip((0, width), ORDERS):
        here = {axis: lax.axis_index(axis) for axis in order}
        pieces = [(line[:, :, start : start + width].reshape(-1, width), here)]
        for axis in order:
            pieces += [
                (to_mate(piece, axis), {**place, axis: 1 - place[axis]}) for piece, place in pieces
            ]
        for piece, place in pieces[1:]:
            whole = lax.dynamic_update_slice(
                whole,
                piece.reshape(count, 1, 1, rows, width),
                (0, place["x"], place["y"], 0, start),
            )
    return whole.reshape(-1, columns)


def halve(grad, order):
    depth, columns = grad.shape
    block = grad.reshape(lax.axis_size("z"), 2, 2, -1, columns)
    dims = (1, 1) if order[0] == "x" else (2, 1)
    for axis, dim in zip(order, dims):
        here = lax.axis_index(axis)
        theirs = lax.dynamic_index_in_dim(block, 1 - here, dim, keepdims=False)
        kept = lax.dynamic_index_in_dim(block, here, dim, keepdims=False)
        received = to_mate(theirs.reshape(-1, columns), axis).reshape(kept.shape)
        block = low(kept.astype(jnp.float32) + received.astype(jnp.float32))
    return block


def start_sums(left, right):
    width = right.shape[1] // 2
    return [
        halve(low(dot_first(left, right[:, start : start + width])), order)
        for start, order in zip((0, width), ORDERS)
    ]


def share_grads(started):
    joined = jnp.concatenate([part for parts in started for part in parts], axis=2)
    summed = lax.psum_scatter(joined, "z", scatter_dimension=0, tiled=True)[0]
    summed = trade_corners(summed).astype(jnp.float32)
    ends = [0]
    for parts in started:
        ends.append(ends[-1] + sum(part.shape[2] for part in parts))
    return [summed[:, start:end] for start, end in zip(ends, ends[1:])]


def after(values, *others):
    return lax.optimization_barrier((values, *others))[0]


def sum_everywhere(values):
    for axis in ("core", "x", "y"):
        values = values + to_mate(values, axis)
    count = lax.axis_size("z")
    step = 1
    while step < count:
        values = values + lax.ppermute(values, "z", [(i, i ^ step) for i in range(count)])
        step *= 2
    return values


def on_pair(
    states,
    text_states,
    norm_gains,
    norm_biases,
    self_qkv,
    self_out,
    cross_query,
    cross_kv,
    cross_out,
    mlp_up,
    mlp_down,
    out_grad,
):
    depth, _, lanes = self_qkv.shape
    pairs = lanes // PAIR
    f32 = jnp.float32
    norm_shard = low(jnp.concatenate([norm_gains, norm_biases], axis=0)).T
    norm_shard = jnp.pad(norm_shard, ((0, 0), (0, 2 * PAIR - norm_shard.shape[1])))
    pieces = [
        low(self_qkv).reshape(depth, 3 * lanes),
        norm_shard,
        low(self_out).T,
        low(cross_query),
        low(cross_kv).reshape(depth, 2 * lanes),
        low(cross_out).T,
        low(mlp_up),
        low(mlp_down).T,
    ]
    shard_one = trade_corners(jnp.concatenate(pieces[:2], axis=1))
    shard = trade_corners(jnp.concatenate(pieces[2:], axis=1))
    second = 5 * lanes
    third = second + mlp_up.shape[1]
    pack_one = fetch(shard_one)
    rows = trade_corners(after(states, shard))
    text_low = trade_corners(after(low(text_states[0]), shard))
    pack_two = fetch(shard[:, :second])
    w_up = fetch(shard[:, second:third])
    w_down = fetch(shard[:, third:])
    w_qkv = pack_one[:, : 3 * lanes]
    norms = pack_one[:, 3 * lanes : 3 * lanes + 6].T.astype(f32)
    gains, biases = norms[:3], norms[3:]
    w_self_out = pack_two[:, :lanes]
    w_query = pack_two[:, lanes : 2 * lanes]
    w_kv = pack_two[:, 2 * lanes : 4 * lanes]
    w_cross_out = pack_two[:, 4 * lanes :]

    def norm_back(values, which, grads):
        _, pull = jax.vjp(normalize, values, gains[which], biases[which])
        return pull(grads)

    def dot(left, right):
        return jnp.dot(left, right, preferred_element_type=f32)

    normed_one = gather_pair(low(normalize(rows, gains[0], biases[0])))
    triple = low(dot(normed_one, w_qkv))
    self_mixed, self_logs = fused_attend(triple, triple, pairs, 2 * pairs, lanes, True)
    grad_rows = trade_corners(after(low(out_grad), self_logs))
    after_self = rows + scatter_pair(self_mixed, lambda part: dot_last(part, w_self_out))
    normed_two = gather_pair(low(normalize(after_self, gains[1], biases[1])))
    queries = low(dot(normed_two, w_query))
    text_pair = low(dot(text_low, w_kv))
    cross_mixed, cross_logs = fused_attend(queries, text_pair, 0, pairs, lanes, False)
    after_cross = after_self + scatter_pair(cross_mixed, lambda part: dot_last(part, w_cross_out))
    normed_three = gather_pair(low(normalize(after_cross, gains[2], biases[2])))
    hidden_pre = dot(normed_three, w_up)
    chance = 0.5 + 0.5 * lax.erf(hidden_pre * math.sqrt(0.5))
    hidden = low(hidden_pre * chance)
    slope = low(
        chance + hidden_pre * jnp.exp(-0.5 * hidden_pre * hidden_pre) / math.sqrt(2 * math.pi)
    )
    branch_grads = gather_pair(grad_rows)
    (down_grad,) = share_grads([start_sums(branch_grads, hidden)])
    layer_out = low(after_cross + scatter_pair(hidden, lambda part: dot_last(part, w_down)))
    pre_grad = low(dot(branch_grads, w_down) * slope.astype(f32))
    (up_grad,) = share_grads([start_sums(normed_three, pre_grad)])
    back_three = scatter_pair(pre_grad, lambda part: dot_last(part, w_up))
    rows_three, gain_three, shift_three = norm_back(after_cross, 2, back_three)
    cross_rows_grad = grad_rows.astype(f32) + rows_three
    cross_grads = gather_pair(low(cross_rows_grad))
    cross_mixed_grad = low(dot(cross_grads, w_cross_out))
    query_grad, key_grad, value_grad = fused_cross_back(
        queries, text_pair, cross_logs, cross_mixed_grad
    )
    pair_grad = jnp.concatenate([key_grad, value_grad], axis=1)
    text_part = dot_last(pair_grad, w_kv)
    text_grad = text_part + to_mate(text_part)
    back_two = scatter_pair(query_grad, lambda part: dot_last(part, w_query))
    rows_two, gain_two, shift_two = norm_back(after_self, 1, back_two)
    self_rows_grad = cross_rows_grad + rows_two
    self_grads = gather_pair(low(self_rows_grad))
    cross_out_grad, query_weight_grad, kv_weight_grad, self_out_grad = share_grads(
        [
            start_sums(cross_grads, cross_mixed),
            start_sums(normed_two, query_grad),
            start_sums(text_low, pair_grad),
            start_sums(self_grads, self_mixed),
        ]
    )
    self_mixed_grad = low(dot(self_grads, w_self_out))
    triple_grad = fused_self_back(triple, self_logs, self_mixed_grad)
    (qkv_grad,) = share_grads([start_sums(normed_one, triple_grad)])
    back_one = scatter_pair(triple_grad, lambda part: dot_last(part, w_qkv))
    rows_one, gain_one, shift_one = norm_back(rows, 0, back_one)
    states_grad = trade_corners(low(self_rows_grad + rows_one)).astype(f32)
    norm_total = sum_everywhere(
        jnp.stack([gain_one, gain_two, gain_three, shift_one, shift_two, shift_three])
    )
    late = (layer_out, text_grad)
    swapped = [lax.ppermute(part, ("core", "y"), [(1, 2), (2, 1)]) for part in late]
    swapped = lax.optimization_barrier((*swapped, norm_total))[:2]
    layer_out, text_grad = [
        jnp.where(at_corner(), theirs, ours).astype(f32) for theirs, ours in zip(swapped, late)
    ]
    width = norm_gains.shape[1]
    place = (lax.axis_index("z") * 2 + lax.axis_index("x")) * 2 + lax.axis_index("core")
    norm_own = lax.dynamic_slice_in_dim(norm_total, place * width, width, 1)
    return (
        layer_out,
        states_grad,
        text_grad[None],
        norm_own[:3],
        norm_own[3:],
        qkv_grad.reshape(depth, 3, lanes),
        self_out_grad.T,
        query_weight_grad,
        kv_weight_grad.reshape(depth, 2, lanes),
        cross_out_grad.T,
        up_grad,
        down_grad.T,
    )


def placements(dp, tensor):
    both = (*dp, *tensor)
    weights = [
        P(dp, None, tensor),
        P(tensor, dp),
        P(dp, tensor),
        P(dp, None, tensor),
        P(tensor, dp),
        P(dp, tensor),
        P(tensor, dp),
    ]
    shared = [P(dp, None, None), P(None, dp), P(None, dp)]
    taken = (P(both, None), *shared, *weights, P(both, None))
    given = (P(both, None), P(both, None), *shared, *weights)
    return taken, given


def solution(mesh):
    dp, tensor = mesh.shape["dp"], mesh.shape["tensor"]
    if tensor == 2 and dp % 4 == 0 and dp & (dp - 1) == 0:
        body = on_pair
        mesh = Mesh(mesh.devices.reshape(dp // 4, 2, 2, 2), ("z", "x", "core", "y"))
        taken, given = placements(("z", "x", "core"), ("y",))
    else:
        body = on_device
        taken, given = placements(("dp",), ("tensor",))
    return jax.shard_map(body, mesh=mesh, in_specs=taken, out_specs=given, check_vma=False)
```
